256 devices in a mesh: space: 64 (over z, y, core), tm: 4 (over x).
Axes of the slice: x: 4, y: 4, z: 8, core: 2. Of those that a mesh axis runs over, the one named last changes fastest.
Arguments:
- precip: float32 [512, 384, 2048], P('tm', 'space'), may hold values from 0.0001 to 0.01
Outputs:
- totals: float32 [384, 2048, 512], P(None, 'space', 'tm')
The draws below stay inside these ranges and needn't reach their ends.
All inputs are finite; a program needn't handle non-finite values.
Results may differ from the reference program's by a relative error of at most 0.00005.
Values sent between devices are 32-bit elements; how exact they have to be, the bound alone decides.
A program may use at most 64 MiB of HBM per device.

```python
import math
import jax
import jax.numpy as jnp

LON = 2048
DAYS = 512
LAT = 384


def steps_of(rng, dims, split, least, high):
    def one(position, blocks):
        steps = jax.random.uniform(jax.random.fold_in(jax.random.fold_in(rng, 6), position), (blocks,), jnp.float32, least / len(split), high / len(split))
        return jnp.repeat(jnp.exp(steps), dims[position] // blocks).reshape((-1,) + (1,) * (len(dims) - position - 1))

    factor_of = one(*split[0])
    for cut in split[1:]:
        factor_of = factor_of * one(*cut)
    return factor_of


def setup_inputs(seed: int = 0) -> dict:
    key_list = jax.random.split(jax.random.key(seed), 2)
    precip = jnp.clip(jnp.exp(math.log(0.01) - 4.6051702 * jax.random.uniform(key_list[0], (DAYS, LAT, LON), jnp.float32) ** steps_of(key_list[0], (DAYS, LAT, LON), ((0, 4), (1, 64)), -0.2, 0.2)), 0.0001, 0.01)
    return {"precip": precip}


def reference(precip):
    running = jnp.cumsum(precip, axis=0)
    return jnp.transpose(running, (1, 2, 0))
```

```python
import functools

import jax
import jax.numpy as jnp
from jax import lax
from jax.experimental import pallas as pl
from jax.experimental.pallas import tpu as pltpu
from jax.sharding import PartitionSpec as P

MESH = pl.DeviceIdType.MESH
Z, Y, C, X = 8, 4, 2, 4
ROWS, DAYS, COLS = 6, 128, 32
WIDE = Y * C * COLS
HOPS = [4, 3, 5, 2, 6, 1, 7, 0]
SIDE = [(2, 1), (2, 0), (1, 0), (3, 0), (1, 1), (3, 1), (0, 1)]


def kernel(x_ref, out_ref, inp, stage, relay, sums, earlier, load_sem,
           xs_sem, xr_sem, ys_sem, yr_sem, zs_sem, zr_sem):
    me = lax.axis_index("space")
    t = lax.axis_index("tm")
    z, yc = me // (Y * C), lax.rem(me, Y * C)
    y, c = yc // C, lax.rem(yc, C)

    def side(dy, dc):
        return lax.rem(y + dy, Y) * C + lax.rem(c + dc, C)

    zs = [lax.rem(z + d, Z) for d in HOPS]
    to = [side(dy, dc) for dy, dc in SIDE]
    source = [side(Y - dy, C - dc) for dy, dc in SIDE]

    loads = []
    for i in range(Z):
        cp = pltpu.make_async_copy(
            x_ref.at[:, :, pl.ds(pl.multiple_of(zs[i] * WIDE, WIDE), WIDE)], inp.at[i], load_sem.at[i])
        cp.start()
        loads.append(cp)

    barrier = pltpu.get_barrier_semaphore()
    for i in range(Z - 1):
        pl.semaphore_signal(barrier, inc=1, device_id={"space": zs[i] * Y * C + yc}, device_id_type=MESH)
    for k in to:
        pl.semaphore_signal(barrier, inc=1, device_id={"space": z * Y * C + k}, device_id_type=MESH)
    for d in range(1, X):
        pl.semaphore_signal(barrier, inc=1, device_id={"tm": lax.rem(t + d, X)}, device_id_type=MESH)

    def add_days(i):
        def row(r, _):
            sums[i, pl.ds(r, 1), :] = jnp.sum(inp[i, r], axis=0, keepdims=True)
            return 0
        lax.fori_loop(0, ROWS, row, 0)

    trades = [[] for _ in range(Z)]
    for i in range(Z):
        loads[i].wait()
        add_days(i)
        if i == 0:
            pl.semaphore_wait(barrier, (Z - 1) + len(SIDE) + (X - 1))
        for d in range(1, X):
            cp = pltpu.make_async_remote_copy(
                sums.at[i], earlier.at[d - 1, i], xs_sem.at[d - 1, i], xr_sem.at[d - 1, i],
                device_id={"tm": lax.rem(t + d, X)}, device_id_type=MESH)
            cp.start()
            trades[i].append(cp)

    lower = (lax.broadcasted_iota(jnp.int32, (DAYS, DAYS), 0)
             >= lax.broadcasted_iota(jnp.int32, (DAYS, DAYS), 1)).astype(jnp.bfloat16)

    def dot(part):
        return jnp.dot(lower, part, preferred_element_type=jnp.float32)

    def totals(i):
        def row(r, _):
            value = inp[i, r]
            high = value.astype(jnp.bfloat16)
            rest = value - high.astype(jnp.float32)
            mid = rest.astype(jnp.bfloat16)
            low = (rest - mid.astype(jnp.float32)).astype(jnp.bfloat16)
            running = dot(low) + dot(mid) + dot(high)
            before = jnp.zeros((1, WIDE), jnp.float32)
            for d in range(1, X):
                got = earlier[d - 1, i, pl.ds(r, 1), :]
                before = before + jnp.where(t >= d, got, jnp.zeros_like(got))
            stage[:, i, r] = (running + before).T.reshape(Y * C, COLS, DAYS)
            return 0
        lax.fori_loop(0, ROWS, row, 0)

    direct, across = [None] * Z, [[None] * len(SIDE) for _ in range(Z)]
    for i in range(Z):
        for cp in trades[i]:
            cp.wait_recv()
        totals(i)
        if HOPS[i]:
            direct[i] = pltpu.make_async_remote_copy(
                stage.at[yc, i], out_ref.at[z, yc], zs_sem.at[i, len(SIDE)], zr_sem.at[i, len(SIDE)],
                device_id={"space": zs[i] * Y * C + yc}, device_id_type=MESH)
            direct[i].start()
        else:
            out_ref[z, yc] = stage[yc, i]
        for j, k in enumerate(to):
            landing = relay.at[j, i] if HOPS[i] else out_ref.at[z, yc]
            across[i][j] = pltpu.make_async_remote_copy(
                stage.at[k, i], landing, ys_sem.at[j, i], yr_sem.at[j, i],
                device_id={"space": z * Y * C + k}, device_id_type=MESH)
            across[i][j].start()

    onward = []
    for i in range(Z):
        for j in range(len(SIDE)):
            across[i][j].wait_recv()
            if HOPS[i]:
                cp = pltpu.make_async_remote_copy(
                    relay.at[j, i], out_ref.at[z, source[j]], zs_sem.at[i, j], zr_sem.at[i, j],
                    device_id={"space": zs[i] * Y * C + yc}, device_id_type=MESH)
                cp.start()
                onward.append(cp)

    for i in range(Z):
        for cp in trades[i] + across[i]:
            cp.wait_send()
    for cp in direct[:-1] + onward:
        cp.wait()


def per_device(precip):
    rows_first = jnp.transpose(precip, (1, 0, 2))
    side = len(SIDE)
    out = pl.pallas_call(
        kernel,
        name="rechunk",
        out_shape=jax.ShapeDtypeStruct((Z, Y * C, ROWS, COLS, DAYS), jnp.float32),
        in_specs=[pl.BlockSpec(memory_space=pltpu.HBM)],
        out_specs=pl.BlockSpec(memory_space=pltpu.VMEM),
        scratch_shapes=[
            pltpu.VMEM((Z, ROWS, DAYS, WIDE), jnp.float32),
            pltpu.VMEM((Y * C, Z, ROWS, COLS, DAYS), jnp.float32),
            pltpu.VMEM((side, Z - 1, ROWS, COLS, DAYS), jnp.float32),
            pltpu.VMEM((Z, ROWS, WIDE), jnp.float32),
            pltpu.VMEM((X - 1, Z, ROWS, WIDE), jnp.float32),
            pltpu.SemaphoreType.DMA((Z,)),
            pltpu.SemaphoreType.DMA((X - 1, Z)),
            pltpu.SemaphoreType.DMA((X - 1, Z)),
            pltpu.SemaphoreType.DMA((side, Z)),
            pltpu.SemaphoreType.DMA((side, Z)),
            pltpu.SemaphoreType.DMA((Z, side + 1)),
            pltpu.SemaphoreType.DMA((Z, side + 1)),
        ],
        compiler_params=pltpu.CompilerParams(
            collective_id=0, has_side_effects=True, vmem_limit_bytes=46 * 2**20),
    )(rows_first)
    return out.reshape(Z * Y * C * ROWS, COLS, DAYS)


def solution(mesh):
    return jax.shard_map(
        per_device, mesh=mesh, in_specs=(P("tm", "space", None),),
        out_specs=P(None, "space", "tm"), check_vma=False)
```

```python
import jax
import jax.numpy as jnp
from jax import lax
from jax.experimental import pallas as pl
from jax.experimental.pallas import tpu as pltpu
from jax.sharding import PartitionSpec as P

MESH = pl.DeviceIdType.MESH
Z, Y, C, X = 8, 4, 2, 4
ROWS, DAYS, COLS, LANES = 6, 128, 32, 128
WIDE = Y * C * COLS
HOPS = [4, 3, 5, 2, 6, 1, 7, 0]
EARLY = 3
WAVES = [(1, 2), (3, 4), (0,), (5, 6), (7,)]
ORDER = [i for wave in WAVES for i in wave]
SIDE = [(2, 1), (2, 0), (1, 0), (3, 0), (1, 1), (3, 1), (0, 1)]
S = len(SIDE)
FINE = 1
UNROLL = 3


def kernel(x_ref, out_ref, inp, stage, relay, first, sums, earlier, late, late_in, column,
           ahead_sem, load_sem, xs_sem, xr_sem, ys_sem, fine_sem, wave_sem, zs_sem, early_sem, direct_sem, onward_sem,
           ls_sem, lr_sem):
    me = lax.axis_index("space")
    t = lax.axis_index("tm")
    z, yc = me // (Y * C), lax.rem(me, Y * C)
    y, c = yc // C, lax.rem(yc, C)

    def side(dy, dc):
        return lax.rem(y + dy, Y) * C + lax.rem(c + dc, C)

    zs = [lax.rem(z + d, Z) for d in HOPS]
    to = [side(dy, dc) for dy, dc in SIDE]
    source = [side(Y - dy, C - dc) for dy, dc in SIDE]
    half = pl.multiple_of(yc // C // 2 * LANES, LANES)
    within = pl.multiple_of(lax.rem(yc, LANES // COLS) * COLS, COLS)

    def load(i, start, width, sem):
        pltpu.make_async_copy(
            x_ref.at[:, :, pl.ds(pl.multiple_of(zs[i] * WIDE + start, LANES), width)],
            inp.at[i, :, :, pl.ds(start, width)], sem).start()

    for i in range(EARLY):
        load(i, half, LANES, ahead_sem.at[i])
    for i in range(Z):
        if i < EARLY:
            load(i, pl.multiple_of(LANES - half, LANES), LANES, load_sem)
        else:
            load(i, 0, WIDE, load_sem)

    barrier = pltpu.get_barrier_semaphore()
    for i in range(Z - 1):
        pl.semaphore_signal(barrier, inc=1, device_id={"space": zs[i] * Y * C + yc}, device_id_type=MESH)
    for k in to:
        pl.semaphore_signal(barrier, inc=1, device_id={"space": z * Y * C + k}, device_id_type=MESH)
    for d in range(1, X):
        pl.semaphore_signal(barrier, inc=1, device_id={"tm": lax.rem(t + d, X)}, device_id_type=MESH)

    lower = (lax.broadcasted_iota(jnp.int32, (DAYS, DAYS), 0)
             >= lax.broadcasted_iota(jnp.int32, (DAYS, DAYS), 1)).astype(jnp.bfloat16)

    def dot(part):
        return jnp.dot(lower, part, preferred_element_type=jnp.float32)

    def over_days(value):
        high = value.astype(jnp.bfloat16)
        rest = value - high.astype(jnp.float32)
        mid = rest.astype(jnp.bfloat16)
        low = (rest - mid.astype(jnp.float32)).astype(jnp.bfloat16)
        return dot(low) + dot(mid) + dot(high)

    def each_row(body, unroll):
        def step(r, carry):
            body(r)
            return carry
        lax.fori_loop(0, ROWS, step, 0, unroll=unroll)

    def own_block(i):
        def row(r):
            first[i, r] = over_days(inp[i, r, :, pl.ds(half, LANES)]).T
        each_row(row, ROWS)

    def add_days(i):
        def row(r):
            sums[i, pl.ds(r, 1), :] = jnp.sum(inp[i, r], axis=0, keepdims=True)
        each_row(row, 1)

    def before(i, rows):
        total = jnp.zeros((1, WIDE), jnp.float32)
        for d in range(1, X):
            got = earlier[d - 1, i, rows, :]
            total = total + jnp.where(t >= d, got, jnp.zeros_like(got))
        return total

    def totals(i):
        def row(r):
            running = over_days(inp[i, r]) + before(i, pl.ds(r, 1))
            stage[:, i, r] = running.T.reshape(Y * C, COLS, DAYS)
        each_row(row, UNROLL)

    def send(src, dst, send_sem, recv_sem, **device):
        pltpu.make_async_remote_copy(
            src, dst, send_sem, recv_sem, device_id=device, device_id_type=MESH).start()

    def arrived(ref, sem):
        pltpu.make_async_remote_copy(ref, ref, sem, sem, device_id={"space": me}, device_id_type=MESH).wait_recv()

    def along_z(i):
        return zs[i] * Y * C + yc

    for i in range(EARLY):
        arrived(inp.at[i, :, :, 0:LANES], ahead_sem.at[i])
        own_block(i)
        if i == 0:
            pl.semaphore_wait(barrier, (Z - 1) + S + (X - 1))
        send(first.at[i, :, pl.ds(within, COLS), :], out_ref.at[z, yc], zs_sem, early_sem.at[i], space=along_z(i))

    arrived(x_ref.at[:, :, 0:(2 * Z - EARLY) * LANES], load_sem)
    for i in ORDER:
        add_days(i)
        for d in range(1, X):
            send(sums.at[i], earlier.at[d - 1, i], xs_sem, xr_sem.at[i], tm=lax.rem(t + d, X))

    for w, wave in enumerate(WAVES):
        for i in wave:
            arrived(earlier.at[:, i], xr_sem.at[i])
            if i < EARLY:
                total = before(i, slice(0, ROWS))
                late[i] = jnp.zeros((8, LANES), jnp.float32)
                late[i, 0:ROWS] = jnp.where(half == 0, total[:, :LANES], total[:, LANES:])
            totals(i)
            if i < EARLY:
                send(late.at[i], late_in.at[i], ls_sem, lr_sem.at[i], space=along_z(i))
            elif HOPS[i]:
                send(stage.at[yc, i], out_ref.at[z, yc], zs_sem, direct_sem, space=along_z(i))
            else:
                out_ref[z, yc] = stage[yc, i]
        for j, k in enumerate(to):
            sem = fine_sem.at[w, j] if w < FINE else wave_sem.at[w - FINE]
            for i in wave:
                landing = relay.at[j, i] if HOPS[i] else out_ref.at[z, yc]
                send(stage.at[k, i], landing, ys_sem, sem, space=z * Y * C + k)

    for w, wave in enumerate(WAVES):
        if w >= FINE:
            arrived(stage.at[0:S, 0:len(wave)], wave_sem.at[w - FINE])
        for j in range(S):
            if w < FINE:
                arrived(stage.at[0, 0:len(wave)], fine_sem.at[w, j])
            for i in wave:
                if HOPS[i]:
                    send(relay.at[j, i], out_ref.at[z, source[j]], zs_sem, onward_sem, space=along_z(i))

    for i in range(EARLY):
        arrived(stage.at[0, 0], early_sem.at[i])
        arrived(late_in.at[i], lr_sem.at[i])
        column[i] = late_in[i].T
        origin = lax.rem(z + Z - HOPS[i], Z)
        for r in range(ROWS):
            out_ref[origin, yc, r] += column[i, pl.ds(within, COLS), r:r + 1]

    arrived(earlier, xs_sem)
    arrived(late, ls_sem)
    arrived(stage.at[0:S], ys_sem)
    arrived(stage.at[0, 0:Z - 1 - EARLY], direct_sem)
    arrived(stage.at[0:Z - 1], zs_sem)
    arrived(relay, onward_sem)


def per_device(precip):
    block = (ROWS, COLS, DAYS)
    out = pl.pallas_call(
        kernel,
        name="rechunk",
        out_shape=jax.ShapeDtypeStruct((Z, Y * C, *block), jnp.float32),
        in_specs=[pl.BlockSpec(memory_space=pl.ANY)],
        out_specs=pl.BlockSpec(memory_space=pltpu.VMEM),
        scratch_shapes=[
            pltpu.VMEM((Z, ROWS, DAYS, WIDE), jnp.float32),
            pltpu.VMEM((Y * C, Z, *block), jnp.float32),
            pltpu.VMEM((S, Z - 1, *block), jnp.float32),
            pltpu.VMEM((EARLY, ROWS, LANES, DAYS), jnp.float32),
            pltpu.VMEM((Z, ROWS, WIDE), jnp.float32),
            pltpu.VMEM((X - 1, Z, ROWS, WIDE), jnp.float32),
            pltpu.VMEM((EARLY, 8, LANES), jnp.float32),
            pltpu.VMEM((EARLY, 8, LANES), jnp.float32),
            pltpu.VMEM((EARLY, LANES, 8), jnp.float32),
            pltpu.SemaphoreType.DMA((EARLY,)),
            pltpu.SemaphoreType.DMA,
            pltpu.SemaphoreType.DMA,
            pltpu.SemaphoreType.DMA((Z,)),
            pltpu.SemaphoreType.DMA,
            pltpu.SemaphoreType.DMA((FINE, S)),
            pltpu.SemaphoreType.DMA((len(WAVES) - FINE,)),
            pltpu.SemaphoreType.DMA,
            pltpu.SemaphoreType.DMA((EARLY,)),
            pltpu.SemaphoreType.DMA,
            pltpu.SemaphoreType.DMA,
            pltpu.SemaphoreType.DMA,
            pltpu.SemaphoreType.DMA((EARLY,)),
        ],
        compiler_params=pltpu.CompilerParams(
            collective_id=0, has_side_effects=True, vmem_limit_bytes=46 * 2**20),
    )(jnp.transpose(precip, (1, 0, 2)))
    return out.reshape(Z * Y * C * ROWS, COLS, DAYS)


def solution(mesh):
    return jax.shard_map(
        per_device, mesh=mesh, in_specs=(P("tm", "space", None),),
        out_specs=P(None, "space", "tm"), check_vma=False)
```

```python
import jax
import jax.numpy as jnp
from jax import lax
from jax.experimental import pallas as pl
from jax.experimental.pallas import tpu as pltpu
from jax.sharding import PartitionSpec as P

MESH = pl.DeviceIdType.MESH
Z, Y, C, X = 8, 4, 2, 4
ROWS, DAYS, COLS, LANES = 6, 128, 32, 128
WIDE = Y * C * COLS
HOPS = [1, 7, 2, 6, 3, 5, 4, 0]
EARLY = 4
WAVES = [(4, 5), (6,), (2, 3), (0, 1), (7,)]
ORDER = [i for wave in WAVES for i in wave]
SIDE = [(2, 1), (2, 0), (1, 0), (3, 0), (1, 1), (3, 1), (0, 1)]
S = len(SIDE)
FINE = 1
UNROLL = 3


def kernel(x_ref, out_ref, inp, stage, relay, first, sums, earlier, late, late_in, column,
           ahead_sem, load_sem, xs_sem, xr_sem, ys_sem, fine_sem, wave_sem, zs_sem, early_sem, direct_sem, onward_sem,
           ls_sem, lr_sem, seen, beside, core_seen, days_seen):
    me = lax.axis_index("space")
    t = lax.axis_index("tm")
    z, yc = me // (Y * C), lax.rem(me, Y * C)
    y, c = yc // C, lax.rem(yc, C)

    def side(dy, dc):
        return lax.rem(y + dy, Y) * C + lax.rem(c + dc, C)

    zs = [lax.rem(z + d, Z) for d in HOPS]
    to = [side(dy, dc) for dy, dc in SIDE]
    source = [side(Y - dy, C - dc) for dy, dc in SIDE]
    half = pl.multiple_of(yc // C // 2 * LANES, LANES)
    within = pl.multiple_of(lax.rem(yc, LANES // COLS) * COLS, COLS)

    def load(i, start, width, sem):
        pltpu.make_async_copy(
            x_ref.at[:, :, pl.ds(pl.multiple_of(zs[i] * WIDE + start, LANES), width)],
            inp.at[i, :, :, pl.ds(start, width)], sem).start()

    for i in range(EARLY):
        load(i, half, LANES, ahead_sem.at[i])
    for i in range(Z):
        if i < EARLY:
            load(i, pl.multiple_of(LANES - half, LANES), LANES, load_sem)
        else:
            load(i, 0, WIDE, load_sem)

    def tell(sem, **device):
        pl.semaphore_signal(sem, inc=1, device_id=device, device_id_type=MESH)

    up, down = (lax.rem(z + d, Z) * Y * C + yc for d in (1, Z - 1))
    left, right, partner = (z * Y * C + side(dy, dc) for dy, dc in ((1, 0), (Y - 1, 0), (0, 1)))
    barrier = pltpu.get_barrier_semaphore()
    for k in (up, down, left, right, partner):
        tell(barrier, space=k)
    for d in (1, X - 1):
        tell(barrier, tm=lax.rem(t + d, X))

    lower = (lax.broadcasted_iota(jnp.int32, (DAYS, DAYS), 0)
             >= lax.broadcasted_iota(jnp.int32, (DAYS, DAYS), 1)).astype(jnp.bfloat16)

    def dot(part):
        return jnp.dot(lower, part, preferred_element_type=jnp.float32)

    def over_days(value):
        high = value.astype(jnp.bfloat16)
        rest = value - high.astype(jnp.float32)
        mid = rest.astype(jnp.bfloat16)
        low = (rest - mid.astype(jnp.float32)).astype(jnp.bfloat16)
        return dot(low) + dot(mid) + dot(high)

    def each_row(body, unroll):
        def step(r, carry):
            body(r)
            return carry
        lax.fori_loop(0, ROWS, step, 0, unroll=unroll)

    def own_block(i):
        def row(r):
            first[i, r] = over_days(inp[i, r, :, pl.ds(half, LANES)]).T
        each_row(row, ROWS)

    def add_days(i):
        def row(r):
            sums[i, pl.ds(r, 1), :] = jnp.sum(inp[i, r], axis=0, keepdims=True)
        each_row(row, 1)

    def before(i, rows):
        total = jnp.zeros((1, WIDE), jnp.float32)
        for d in range(1, X):
            got = earlier[d - 1, i, rows, :]
            total = total + jnp.where(t >= d, got, jnp.zeros_like(got))
        return total

    def totals(i):
        def row(r):
            running = over_days(inp[i, r]) + before(i, pl.ds(r, 1))
            stage[:, i, r] = running.T.reshape(Y * C, COLS, DAYS)
        each_row(row, UNROLL)

    def send(src, dst, send_sem, recv_sem, **device):
        pltpu.make_async_remote_copy(
            src, dst, send_sem, recv_sem, device_id=device, device_id_type=MESH).start()

    def arrived(ref, sem):
        pltpu.make_async_remote_copy(ref, ref, sem, sem, device_id={"space": me}, device_id_type=MESH).wait_recv()

    def along_z(i):
        return zs[i] * Y * C + yc

    for i in range(EARLY):
        arrived(inp.at[i, :, :, 0:LANES], ahead_sem.at[i])
        own_block(i)
        if i == 0:
            pl.semaphore_wait(barrier, 7)
            tell(seen.at[0], space=down)
            tell(seen.at[1], space=up)
            tell(beside, space=left)
            tell(beside, space=right)
            tell(days_seen, tm=lax.rem(t + X - 1, X))
        if i == 2:
            pl.semaphore_wait(seen.at[0], 1)
            tell(seen.at[2], space=down)
        if i == 3:
            pl.semaphore_wait(seen.at[1], 1)
            tell(seen.at[3], space=up)
        send(first.at[i, :, pl.ds(within, COLS), :], out_ref.at[z, yc], zs_sem, early_sem.at[i], space=along_z(i))

    pl.semaphore_wait(seen.at[2], 1)
    tell(seen.at[4], space=down)
    pl.semaphore_wait(beside, 2)
    tell(core_seen, space=partner)
    pl.semaphore_wait(days_seen, 1)

    arrived(x_ref.at[:, :, 0:(2 * Z - EARLY) * LANES], load_sem)
    for i in ORDER:
        add_days(i)
        for d in range(1, X):
            send(sums.at[i], earlier.at[d - 1, i], xs_sem, xr_sem.at[i], tm=lax.rem(t + d, X))

    pl.semaphore_wait(seen.at[3], 1)
    pl.semaphore_wait(seen.at[4], 1)
    pl.semaphore_wait(core_seen, 1)
    for w, wave in enumerate(WAVES):
        for i in wave:
            arrived(earlier.at[:, i], xr_sem.at[i])
            if i < EARLY:
                total = before(i, slice(0, ROWS))
                late[i] = jnp.zeros((8, LANES), jnp.float32)
                late[i, 0:ROWS] = jnp.where(half == 0, total[:, :LANES], total[:, LANES:])
            totals(i)
            if i < EARLY:
                send(late.at[i], late_in.at[i], ls_sem, lr_sem.at[i], space=along_z(i))
            elif HOPS[i]:
                send(stage.at[yc, i], out_ref.at[z, yc], zs_sem, direct_sem, space=along_z(i))
            else:
                out_ref[z, yc] = stage[yc, i]
        for j, k in enumerate(to):
            sem = fine_sem.at[w, j] if w < FINE else wave_sem.at[w - FINE]
            for i in wave:
                landing = relay.at[j, i] if HOPS[i] else out_ref.at[z, yc]
                send(stage.at[k, i], landing, ys_sem, sem, space=z * Y * C + k)

    for w, wave in enumerate(WAVES):
        if w >= FINE:
            arrived(stage.at[0:S, 0:len(wave)], wave_sem.at[w - FINE])
        for j in range(S):
            if w < FINE:
                arrived(stage.at[0, 0:len(wave)], fine_sem.at[w, j])
            for i in wave:
                if HOPS[i]:
                    send(relay.at[j, i], out_ref.at[z, source[j]], zs_sem, onward_sem, space=along_z(i))

    for i in range(EARLY):
        arrived(stage.at[0, 0], early_sem.at[i])
        arrived(late_in.at[i], lr_sem.at[i])
        column[i] = late_in[i].T
        origin = lax.rem(z + Z - HOPS[i], Z)
        for r in range(ROWS):
            out_ref[origin, yc, r] += column[i, pl.ds(within, COLS), r:r + 1]

    arrived(earlier, xs_sem)
    arrived(late, ls_sem)
    arrived(stage.at[0:S], ys_sem)
    arrived(stage.at[0, 0:Z - 1 - EARLY], direct_sem)
    arrived(stage.at[0:Z - 1], zs_sem)
    arrived(relay, onward_sem)


def per_device(precip):
    block = (ROWS, COLS, DAYS)
    out = pl.pallas_call(
        kernel,
        name="rechunk",
        out_shape=jax.ShapeDtypeStruct((Z, Y * C, *block), jnp.float32),
        in_specs=[pl.BlockSpec(memory_space=pl.ANY)],
        out_specs=pl.BlockSpec(memory_space=pltpu.VMEM),
        scratch_shapes=[
            pltpu.VMEM((Z, ROWS, DAYS, WIDE), jnp.float32),
            pltpu.VMEM((Y * C, Z, *block), jnp.float32),
            pltpu.VMEM((S, Z - 1, *block), jnp.float32),
            pltpu.VMEM((EARLY, ROWS, LANES, DAYS), jnp.float32),
            pltpu.VMEM((Z, ROWS, WIDE), jnp.float32),
            pltpu.VMEM((X - 1, Z, ROWS, WIDE), jnp.float32),
            pltpu.VMEM((EARLY, 8, LANES), jnp.float32),
            pltpu.VMEM((EARLY, 8, LANES), jnp.float32),
            pltpu.VMEM((EARLY, LANES, 8), jnp.float32),
            pltpu.SemaphoreType.DMA((EARLY,)),
            pltpu.SemaphoreType.DMA,
            pltpu.SemaphoreType.DMA,
            pltpu.SemaphoreType.DMA((Z,)),
            pltpu.SemaphoreType.DMA,
            pltpu.SemaphoreType.DMA((FINE, S)),
            pltpu.SemaphoreType.DMA((len(WAVES) - FINE,)),
            pltpu.SemaphoreType.DMA,
            pltpu.SemaphoreType.DMA((EARLY,)),
            pltpu.SemaphoreType.DMA,
            pltpu.SemaphoreType.DMA,
            pltpu.SemaphoreType.DMA,
            pltpu.SemaphoreType.DMA((EARLY,)),
            pltpu.SemaphoreType.REGULAR((5,)),
            pltpu.SemaphoreType.REGULAR,
            pltpu.SemaphoreType.REGULAR,
            pltpu.SemaphoreType.REGULAR,
        ],
        compiler_params=pltpu.CompilerParams(
            collective_id=0, has_side_effects=True, vmem_limit_bytes=46 * 2**20),
    )(jnp.transpose(precip, (1, 0, 2)))
    return out.reshape(Z * Y * C * ROWS, COLS, DAYS)


def solution(mesh):
    return jax.shard_map(
        per_device, mesh=mesh, in_specs=(P("tm", "space", None),),
        out_specs=P(None, "space", "tm"), check_vma=False)
```

```python
import jax
import jax.numpy as jnp
from jax import lax
from jax.experimental import pallas as pl
from jax.experimental.pallas import tpu as pltpu
from jax.sharding import PartitionSpec as P

MESH = pl.DeviceIdType.MESH
Z, Y, C, X = 8, 4, 2, 4
ROWS, DAYS, COLS, LANES = 6, 128, 32, 128
WIDE = Y * C * COLS
HOPS = [1, 7, 2, 6, 3, 5, 4, 0]
EARLY = 4
WAVES = [(4, 5), (6,), (2, 3), (0, 1), (7,)]
ORDER = [i for wave in WAVES for i in wave]
SIDE = [(2, 1), (2, 0), (1, 0), (3, 0), (1, 1), (3, 1), (0, 1)]
S = len(SIDE)
FINE = 1
UNROLL = 6


def kernel(x_ref, out_ref, inp, stage, relay, first, sums, earlier, late, late_in, column,
           ahead_sem, load_sem, xs_sem, xr_sem, ys_sem, fine_sem, wave_sem, zs_sem, early_sem, direct_sem, onward_sem,
           ls_sem, lr_sem, seen, beside, core_seen, days_seen):
    me = lax.axis_index("space")
    t = lax.axis_index("tm")
    z, yc = me // (Y * C), lax.rem(me, Y * C)
    y, c = yc // C, lax.rem(yc, C)

    def side(dy, dc):
        return lax.rem(y + dy, Y) * C + lax.rem(c + dc, C)

    zs = [lax.rem(z + d, Z) for d in HOPS]
    to = [side(dy, dc) for dy, dc in SIDE]
    source = [side(Y - dy, C - dc) for dy, dc in SIDE]
    half = pl.multiple_of(yc // C // 2 * LANES, LANES)
    within = pl.multiple_of(lax.rem(yc, LANES // COLS) * COLS, COLS)

    def load(i, start, width, sem):
        pltpu.make_async_copy(
            x_ref.at[:, :, pl.ds(pl.multiple_of(zs[i] * WIDE + start, LANES), width)],
            inp.at[i, :, :, pl.ds(start, width)], sem).start()

    def tell(sem, **device):
        pl.semaphore_signal(sem, inc=1, device_id=device, device_id_type=MESH)

    up, down = (lax.rem(z + d, Z) * Y * C + yc for d in (1, Z - 1))
    left, right, partner = (z * Y * C + side(dy, dc) for dy, dc in ((1, 0), (Y - 1, 0), (0, 1)))
    barrier = pltpu.get_barrier_semaphore()
    for k in (up, down, left, right, partner):
        tell(barrier, space=k)
    for d in (1, X - 1):
        tell(barrier, tm=lax.rem(t + d, X))

    for i in range(EARLY):
        load(i, half, LANES, ahead_sem.at[i])
    for i in range(Z):
        if i < EARLY:
            load(i, pl.multiple_of(LANES - half, LANES), LANES, load_sem)
        else:
            load(i, 0, WIDE, load_sem)

    lower = (lax.broadcasted_iota(jnp.int32, (DAYS, DAYS), 0)
             >= lax.broadcasted_iota(jnp.int32, (DAYS, DAYS), 1)).astype(jnp.bfloat16)

    def dot(part):
        return jnp.dot(lower, part, preferred_element_type=jnp.float32)

    def over_days(value):
        high = value.astype(jnp.bfloat16)
        rest = value - high.astype(jnp.float32)
        mid = rest.astype(jnp.bfloat16)
        low = (rest - mid.astype(jnp.float32)).astype(jnp.bfloat16)
        return dot(low) + dot(mid) + dot(high)

    def each_row(body, unroll):
        def step(r, carry):
            body(r)
            return carry
        lax.fori_loop(0, ROWS, step, 0, unroll=unroll)

    def own_block(i):
        def row(r):
            first[i, r] = over_days(inp[i, r, :, pl.ds(half, LANES)]).T
        each_row(row, ROWS)

    def add_days(i):
        def row(r):
            sums[i, pl.ds(r, 1), :] = jnp.sum(inp[i, r], axis=0, keepdims=True)
        each_row(row, 1)

    def before(i, rows):
        total = jnp.zeros((1, WIDE), jnp.float32)
        for d in range(1, X):
            got = earlier[d - 1, i, rows, :]
            total = total + jnp.where(t >= d, got, jnp.zeros_like(got))
        return total

    def totals(i):
        def row(r):
            running = over_days(inp[i, r]) + before(i, pl.ds(r, 1))
            stage[:, i, r] = running.T.reshape(Y * C, COLS, DAYS)
        each_row(row, UNROLL)

    def send(src, dst, send_sem, recv_sem, **device):
        pltpu.make_async_remote_copy(
            src, dst, send_sem, recv_sem, device_id=device, device_id_type=MESH).start()

    def arrived(ref, sem):
        pltpu.make_async_remote_copy(ref, ref, sem, sem, device_id={"space": me}, device_id_type=MESH).wait_recv()

    def along_z(i):
        return zs[i] * Y * C + yc

    for i in range(EARLY):
        arrived(inp.at[i, :, :, 0:LANES], ahead_sem.at[i])
        own_block(i)
        if i == 0:
            pl.semaphore_wait(barrier, 7)
            tell(seen.at[0], space=down)
            tell(seen.at[1], space=up)
            tell(beside, space=left)
            tell(beside, space=right)
            tell(days_seen, tm=lax.rem(t + X - 1, X))
        if i == 2:
            pl.semaphore_wait(seen.at[0], 1)
            tell(seen.at[2], space=down)
        if i == 3:
            pl.semaphore_wait(seen.at[1], 1)
            tell(seen.at[3], space=up)
        send(first.at[i, :, pl.ds(within, COLS), :], out_ref.at[z, yc], zs_sem, early_sem.at[i], space=along_z(i))

    pl.semaphore_wait(seen.at[2], 1)
    tell(seen.at[4], space=down)
    pl.semaphore_wait(beside, 2)
    tell(core_seen, space=partner)
    pl.semaphore_wait(days_seen, 1)

    arrived(x_ref.at[:, :, 0:(2 * Z - EARLY) * LANES], load_sem)
    for i in ORDER:
        add_days(i)
        for d in range(1, X):
            send(sums.at[i], earlier.at[d - 1, i], xs_sem, xr_sem.at[i], tm=lax.rem(t + d, X))

    pl.semaphore_wait(seen.at[3], 1)
    pl.semaphore_wait(seen.at[4], 1)
    pl.semaphore_wait(core_seen, 1)
    for w, wave in enumerate(WAVES):
        for i in wave:
            arrived(earlier.at[:, i], xr_sem.at[i])
            if i < EARLY:
                total = before(i, slice(0, ROWS))
                late[i] = jnp.zeros((8, LANES), jnp.float32)
                late[i, 0:ROWS] = jnp.where(half == 0, total[:, :LANES], total[:, LANES:])
            totals(i)
            if i < EARLY:
                send(late.at[i], late_in.at[i], ls_sem, lr_sem.at[i], space=along_z(i))
            elif HOPS[i]:
                send(stage.at[yc, i], out_ref.at[z, yc], zs_sem, direct_sem, space=along_z(i))
            else:
                out_ref[z, yc] = stage[yc, i]
        for j, k in enumerate(to):
            sem = fine_sem.at[w, j] if w < FINE else wave_sem.at[w - FINE]
            for i in wave:
                landing = relay.at[j, i] if HOPS[i] else out_ref.at[z, yc]
                send(stage.at[k, i], landing, ys_sem, sem, space=z * Y * C + k)

    for w, wave in enumerate(WAVES):
        if w >= FINE:
            arrived(stage.at[0:S, 0:len(wave)], wave_sem.at[w - FINE])
        for j in range(S):
            if w < FINE:
                arrived(stage.at[0, 0:len(wave)], fine_sem.at[w, j])
            for i in wave:
                if HOPS[i]:
                    send(relay.at[j, i], out_ref.at[z, source[j]], zs_sem, onward_sem, space=along_z(i))

    for i in range(EARLY):
        arrived(stage.at[0, 0], early_sem.at[i])
        arrived(late_in.at[i], lr_sem.at[i])
        column[i] = late_in[i].T
        origin = lax.rem(z + Z - HOPS[i], Z)
        for r in range(ROWS):
            out_ref[origin, yc, r] += column[i, pl.ds(within, COLS), r:r + 1]

    arrived(earlier, xs_sem)
    arrived(late, ls_sem)
    arrived(stage.at[0:S], ys_sem)
    arrived(stage.at[0, 0:Z - 1 - EARLY], direct_sem)
    arrived(stage.at[0:Z - 1], zs_sem)
    arrived(relay, onward_sem)


def per_device(precip):
    block = (ROWS, COLS, DAYS)
    out = pl.pallas_call(
        kernel,
        name="rechunk",
        out_shape=jax.ShapeDtypeStruct((Z, Y * C, *block), jnp.float32),
        in_specs=[pl.BlockSpec(memory_space=pl.ANY)],
        out_specs=pl.BlockSpec(memory_space=pltpu.VMEM),
        scratch_shapes=[
            pltpu.VMEM((Z, ROWS, DAYS, WIDE), jnp.float32),
            pltpu.VMEM((Y * C, Z, *block), jnp.float32),
            pltpu.VMEM((S, Z - 1, *block), jnp.float32),
            pltpu.VMEM((EARLY, ROWS, LANES, DAYS), jnp.float32),
            pltpu.VMEM((Z, ROWS, WIDE), jnp.float32),
            pltpu.VMEM((X - 1, Z, ROWS, WIDE), jnp.float32),
            pltpu.VMEM((EARLY, 8, LANES), jnp.float32),
            pltpu.VMEM((EARLY, 8, LANES), jnp.float32),
            pltpu.VMEM((EARLY, LANES, 8), jnp.float32),
            pltpu.SemaphoreType.DMA((EARLY,)),
            pltpu.SemaphoreType.DMA,
            pltpu.SemaphoreType.DMA,
            pltpu.SemaphoreType.DMA((Z,)),
            pltpu.SemaphoreType.DMA,
            pltpu.SemaphoreType.DMA((FINE, S)),
            pltpu.SemaphoreType.DMA((len(WAVES) - FINE,)),
            pltpu.SemaphoreType.DMA,
            pltpu.SemaphoreType.DMA((EARLY,)),
            pltpu.SemaphoreType.DMA,
            pltpu.SemaphoreType.DMA,
            pltpu.SemaphoreType.DMA,
            pltpu.SemaphoreType.DMA((EARLY,)),
            pltpu.SemaphoreType.REGULAR((5,)),
            pltpu.SemaphoreType.REGULAR,
            pltpu.SemaphoreType.REGULAR,
            pltpu.SemaphoreType.REGULAR,
        ],
        compiler_params=pltpu.CompilerParams(
            collective_id=0, has_side_effects=True, vmem_limit_bytes=46 * 2**20),
    )(jnp.transpose(precip, (1, 0, 2)))
    return out.reshape(Z * Y * C * ROWS, COLS, DAYS)


def solution(mesh):
    return jax.shard_map(
        per_device, mesh=mesh, in_specs=(P("tm", "space", None),),
        out_specs=P(None, "space", "tm"), check_vma=False)
```

```python
import jax
import jax.numpy as jnp
from jax import lax
from jax.experimental import pallas as pl
from jax.experimental.pallas import tpu as pltpu
from jax.sharding import PartitionSpec as P

MESH = pl.DeviceIdType.MESH
Z, Y, C, X = 8, 4, 2, 4
ROWS, DAYS, COLS, LANES = 6, 128, 32, 128
WIDE = Y * C * COLS
HOPS = [1, 7, 2, 6, 3, 5, 4, 0]
EARLY = 4
WAVES = [(4, 5), (6,), (2, 3), (0, 1), (7,)]
ORDER = [i for wave in WAVES for i in wave]
SIDE = [(2, 1), (2, 0), (1, 0), (3, 0), (1, 1), (3, 1), (0, 1)]
S = len(SIDE)
FINE = 1
UNROLL = 6


def kernel(x_ref, out_ref, inp, stage, relay, first, sums, earlier, late, late_in, column,
           ahead_sem, load_sem, xs_sem, xr_sem, ys_sem, fine_sem, wave_sem, zs_sem, early_sem, direct_sem, onward_sem,
           ls_sem, lr_sem, seen, beside, core_seen, days_seen):
    me = lax.axis_index("space")
    t = lax.axis_index("tm")
    z, yc = me // (Y * C), lax.rem(me, Y * C)
    y, c = yc // C, lax.rem(yc, C)

    def side(dy, dc):
        return lax.rem(y + dy, Y) * C + lax.rem(c + dc, C)

    zs = [lax.rem(z + d, Z) for d in HOPS]
    to = [side(dy, dc) for dy, dc in SIDE]
    source = [side(Y - dy, C - dc) for dy, dc in SIDE]
    half = pl.multiple_of(yc // C // 2 * LANES, LANES)
    within = pl.multiple_of(lax.rem(yc, LANES // COLS) * COLS, COLS)

    def load(i, start, width, sem):
        pltpu.make_async_copy(
            x_ref.at[:, :, pl.ds(pl.multiple_of(zs[i] * WIDE + start, LANES), width)],
            inp.at[i, :, :, pl.ds(start, width)], sem).start()

    def tell(sem, **device):
        pl.semaphore_signal(sem, inc=1, device_id=device, device_id_type=MESH)

    up, down = (lax.rem(z + d, Z) * Y * C + yc for d in (1, Z - 1))
    left, right, partner = (z * Y * C + side(dy, dc) for dy, dc in ((1, 0), (Y - 1, 0), (0, 1)))
    barrier = pltpu.get_barrier_semaphore()
    for k in (up, down, left, right, partner):
        tell(barrier, space=k)
    for d in (1, X - 1):
        tell(barrier, tm=lax.rem(t + d, X))

    for i in range(EARLY):
        load(i, half, LANES, ahead_sem.at[i])
    for i in range(Z):
        if i < EARLY:
            load(i, pl.multiple_of(LANES - half, LANES), LANES, load_sem)
        else:
            load(i, 0, WIDE, load_sem)

    lower = (lax.broadcasted_iota(jnp.int32, (DAYS, DAYS), 0)
             >= lax.broadcasted_iota(jnp.int32, (DAYS, DAYS), 1)).astype(jnp.bfloat16)

    def dot(part):
        return jnp.dot(lower, part, preferred_element_type=jnp.float32)

    def over_days(value):
        high = value.astype(jnp.bfloat16)
        rest = value - high.astype(jnp.float32)
        mid = rest.astype(jnp.bfloat16)
        low = (rest - mid.astype(jnp.float32)).astype(jnp.bfloat16)
        return dot(low) + dot(mid) + dot(high)

    def each_row(body, unroll):
        def step(r, carry):
            body(r)
            return carry
        lax.fori_loop(0, ROWS, step, 0, unroll=unroll)

    def own_block(i):
        def row(r):
            first[i, r] = over_days(inp[i, r, :, pl.ds(half, LANES)]).T
        each_row(row, ROWS)

    def add_days(i):
        def row(r):
            sums[i, pl.ds(r, 1), :] = jnp.sum(inp[i, r], axis=0, keepdims=True)
        each_row(row, 1)

    def before(i, rows):
        total = jnp.zeros((1, WIDE), jnp.float32)
        for d in range(1, X):
            got = earlier[d - 1, i, rows, :]
            total = total + jnp.where(t >= d, got, jnp.zeros_like(got))
        return total

    def totals(i):
        def row(r):
            running = over_days(inp[i, r]) + before(i, pl.ds(r, 1))
            stage[:, i, r] = running.T.reshape(Y * C, COLS, DAYS)
        each_row(row, UNROLL)

    def send(src, dst, send_sem, recv_sem, **device):
        pltpu.make_async_remote_copy(
            src, dst, send_sem, recv_sem, device_id=device, device_id_type=MESH).start()

    def arrived(ref, sem):
        pltpu.make_async_remote_copy(ref, ref, sem, sem, device_id={"space": me}, device_id_type=MESH).wait_recv()

    def along_z(i):
        return zs[i] * Y * C + yc

    for i in range(EARLY):
        arrived(inp.at[i, :, :, 0:LANES], ahead_sem.at[i])
        own_block(i)
        if i == 0:
            pl.semaphore_wait(barrier, 7)
            tell(seen.at[0], space=down)
            tell(seen.at[1], space=up)
            tell(beside, space=left)
            tell(beside, space=right)
            tell(days_seen, tm=lax.rem(t + X - 1, X))
        if i == 2:
            pl.semaphore_wait(seen.at[0], 1)
            tell(seen.at[2], space=down)
        if i == 3:
            pl.semaphore_wait(seen.at[1], 1)
            tell(seen.at[3], space=up)
        send(first.at[i, :, pl.ds(within, COLS), :], out_ref.at[z, yc], zs_sem, early_sem, space=along_z(i))

    pl.semaphore_wait(seen.at[2], 1)
    tell(seen.at[4], space=down)
    pl.semaphore_wait(beside, 2)
    tell(core_seen, space=partner)
    pl.semaphore_wait(days_seen, 1)

    arrived(x_ref.at[:, :, 0:(2 * Z - EARLY) * LANES], load_sem)
    for i in ORDER:
        add_days(i)
        for d in range(1, X):
            send(sums.at[i], earlier.at[d - 1, i], xs_sem, xr_sem.at[i], tm=lax.rem(t + d, X))

    pl.semaphore_wait(seen.at[3], 1)
    pl.semaphore_wait(seen.at[4], 1)
    pl.semaphore_wait(core_seen, 1)
    for w, wave in enumerate(WAVES):
        for i in wave:
            arrived(earlier.at[:, i], xr_sem.at[i])
            if i < EARLY:
                total = before(i, slice(0, ROWS))
                late[i] = jnp.zeros((8, LANES), jnp.float32)
                late[i, 0:ROWS] = jnp.where(half == 0, total[:, :LANES], total[:, LANES:])
            totals(i)
            if i < EARLY:
                send(late.at[i], late_in.at[i], ls_sem, lr_sem, space=along_z(i))
            elif HOPS[i]:
                send(stage.at[yc, i], out_ref.at[z, yc], zs_sem, direct_sem, space=along_z(i))
            else:
                out_ref[z, yc] = stage[yc, i]
        for j, k in enumerate(to):
            sem = fine_sem.at[w, j] if w < FINE else wave_sem.at[w - FINE]
            for i in wave:
                landing = relay.at[j, i] if HOPS[i] else out_ref.at[z, yc]
                send(stage.at[k, i], landing, ys_sem, sem, space=z * Y * C + k)

    for w, wave in enumerate(WAVES):
        if w >= FINE:
            arrived(stage.at[0:S, 0:len(wave)], wave_sem.at[w - FINE])
        for j in range(S):
            if w < FINE:
                arrived(stage.at[0, 0:len(wave)], fine_sem.at[w, j])
            for i in wave:
                if HOPS[i]:
                    send(relay.at[j, i], out_ref.at[z, source[j]], zs_sem, onward_sem, space=along_z(i))

    arrived(stage.at[0, 0:EARLY], early_sem)
    arrived(late_in, lr_sem)
    for i in range(EARLY):
        column[i] = late_in[i].T
        origin = lax.rem(z + Z - HOPS[i], Z)
        for r in range(ROWS):
            out_ref[origin, yc, r] += column[i, pl.ds(within, COLS), r:r + 1]

    arrived(earlier, xs_sem)
    arrived(late, ls_sem)
    arrived(stage.at[0:S], ys_sem)
    arrived(stage.at[0, 0:Z - 1 - EARLY], direct_sem)
    arrived(stage.at[0:Z - 1], zs_sem)
    arrived(relay, onward_sem)


def per_device(precip):
    block = (ROWS, COLS, DAYS)
    out = pl.pallas_call(
        kernel,
        name="rechunk",
        out_shape=jax.ShapeDtypeStruct((Z, Y * C, *block), jnp.float32),
        in_specs=[pl.BlockSpec(memory_space=pl.ANY)],
        out_specs=pl.BlockSpec(memory_space=pltpu.VMEM),
        scratch_shapes=[
            pltpu.VMEM((Z, ROWS, DAYS, WIDE), jnp.float32),
            pltpu.VMEM((Y * C, Z, *block), jnp.float32),
            pltpu.VMEM((S, Z - 1, *block), jnp.float32),
            pltpu.VMEM((EARLY, ROWS, LANES, DAYS), jnp.float32),
            pltpu.VMEM((Z, ROWS, WIDE), jnp.float32),
            pltpu.VMEM((X - 1, Z, ROWS, WIDE), jnp.float32),
            pltpu.VMEM((EARLY, 8, LANES), jnp.float32),
            pltpu.VMEM((EARLY, 8, LANES), jnp.float32),
            pltpu.VMEM((EARLY, LANES, 8), jnp.float32),
            pltpu.SemaphoreType.DMA((EARLY,)),
            pltpu.SemaphoreType.DMA,
            pltpu.SemaphoreType.DMA,
            pltpu.SemaphoreType.DMA((Z,)),
            pltpu.SemaphoreType.DMA,
            pltpu.SemaphoreType.DMA((FINE, S)),
            pltpu.SemaphoreType.DMA((len(WAVES) - FINE,)),
            pltpu.SemaphoreType.DMA,
            pltpu.SemaphoreType.DMA,
            pltpu.SemaphoreType.DMA,
            pltpu.SemaphoreType.DMA,
            pltpu.SemaphoreType.DMA,
            pltpu.SemaphoreType.DMA,
            pltpu.SemaphoreType.REGULAR((5,)),
            pltpu.SemaphoreType.REGULAR,
            pltpu.SemaphoreType.REGULAR,
            pltpu.SemaphoreType.REGULAR,
        ],
        compiler_params=pltpu.CompilerParams(
            collective_id=0, has_side_effects=True, vmem_limit_bytes=46 * 2**20),
    )(jnp.transpose(precip, (1, 0, 2)))
    return out.reshape(Z * Y * C * ROWS, COLS, DAYS)


def solution(mesh):
    return jax.shard_map(
        per_device, mesh=mesh, in_specs=(P("tm", "space", None),),
        out_specs=P(None, "space", "tm"), check_vma=False)
```
